8 devices in a mesh: rep: 1 (over z), dp: 8 (over x, y, core).
Axes of the slice: x: 2, y: 2, z: 1, core: 2. Of those that a mesh axis runs over, the one named last changes fastest.
Arguments:
- x: bfloat16 [8, 2048, 896], P(('rep', 'dp'))
- dy: bfloat16 [8, 2048, 896], P(('rep', 'dp'))
- w_gate: bfloat16 [2, 896, 4864], P(None, 'dp')
- w_up: bfloat16 [2, 896, 4864], P(None, 'dp')
- w_down: bfloat16 [2, 4864, 896], P(None, 'dp')
- m_w_gate: float32 [2, 896, 4864], P(None, 'dp')
- m_w_up: float32 [2, 896, 4864], P(None, 'dp')
- m_w_down: float32 [2, 4864, 896], P(None, 'dp')
- v_w_gate: float32 [2, 896, 4864], P(None, 'dp')
- v_w_up: float32 [2, 896, 4864], P(None, 'dp')
- v_w_down: float32 [2, 4864, 896], P(None, 'dp')
Outputs:
- output 1: bfloat16 [2, 896, 4864], P('rep', 'dp')
- output 2: bfloat16 [2, 896, 4864], P('rep', 'dp')
- output 3: bfloat16 [2, 4864, 896], P('rep', 'dp')
- output 4: float32 [2, 896, 4864], P('rep', 'dp')
- output 5: float32 [2, 896, 4864], P('rep', 'dp')
- output 6: float32 [2, 4864, 896], P('rep', 'dp')
- output 7: float32 [2, 896, 4864], P('rep', 'dp')
- output 8: float32 [2, 896, 4864], P('rep', 'dp')
- output 9: float32 [2, 4864, 896], P('rep', 'dp')
All inputs are finite; a program needn't handle non-finite values.
Results may differ from the reference program's by a relative error of at most 0.0277.
Values are sent between devices in bfloat16 or wider.
A program may use at most 2 GiB of HBM per device.

```python
import jax
import jax.numpy as jnp
from jax import lax

SEQUENCES = 8
TOKENS = 2048
D = 896
FF = 4864
LAYERS = 2
NAMES = ("w_gate", "w_up", "w_down")
SHAPES = {"w_gate": (LAYERS, D, FF), "w_up": (LAYERS, D, FF), "w_down": (LAYERS, FF, D)}


def bump(key, n, height):
    away = (jnp.arange(n, dtype=jnp.int32) - jax.random.randint(key, (), 0, n, jnp.int32)) % n
    return jnp.where(away < n // 8, height, 1.0)


def together(key, own, strength):
    shared = jax.random.normal(key, own.shape[1:], jnp.float32)
    return (own + strength * shared) * lax.rsqrt(1 + strength * strength)


def setup_inputs(seed: int = 0, part: int = 0) -> dict:
    kx, kdy, ka, kb, kz, kf, kh, kl, *keys = jax.random.split(jax.random.key(seed), 8 + 3 * len(NAMES))
    kx, kdy, ka, kb = (jax.random.fold_in(k, part) for k in (kx, kdy, ka, kb))
    kw, km, kv = (keys[i::3] for i in range(3))
    shape = (SEQUENCES, TOKENS, D)
    much_x, much_dy = jax.random.uniform(kz, (2,), jnp.float32, 0.0, 1.0)
    loud = 2.0 ** jax.random.uniform(jax.random.fold_in(kz, 1), (), jnp.float32, -1.0, 2.0)
    layers = 2.0 ** jax.random.uniform(kl, (LAYERS, 1, 1), jnp.float32, -1.0, 1.0)
    x = together(ka, jax.random.normal(kx, shape, jnp.float32), much_x) * bump(kf, D, 4.0)
    dy = together(kb, jax.random.normal(kdy, shape, jnp.float32), much_dy)
    drawn = {"x": x.astype(jnp.bfloat16), "dy": (loud * dy * (SEQUENCES * TOKENS) ** -0.5).astype(jnp.bfloat16)}
    for key, name in zip(kw, NAMES, strict=True):
        w = jax.random.normal(key, SHAPES[name], jnp.float32) * SHAPES[name][1] ** -0.5
        drawn[name] = (w * {"w_gate": 1.0, "w_up": bump(kh, FF, 4.0), "w_down": layers}[name]).astype(jnp.bfloat16)
    for key, name in zip(km, NAMES, strict=True):
        drawn[f"m_{name}"] = 0.1 * jax.random.normal(key, SHAPES[name], jnp.float32)
    for key, name in zip(kv, NAMES, strict=True):
        drawn[f"v_{name}"] = jax.random.uniform(key, SHAPES[name], jnp.float32, 0.005, 0.015)
    return drawn


def matmul(a, w):
    return jnp.dot(a, w, preferred_element_type=jnp.float32).astype(jnp.bfloat16)


def normed(h):
    wide = h.astype(jnp.float32)
    scale = lax.rsqrt(jnp.mean(wide**2, -1, keepdims=True) + 1e-6)
    return (wide * scale).astype(jnp.bfloat16)


def layer(h, w):
    a = normed(h)
    gate = jnp.dot(a, w["w_gate"], preferred_element_type=jnp.float32)
    up = jnp.dot(a, w["w_up"], preferred_element_type=jnp.float32)
    return h + matmul((jax.nn.silu(gate) * up).astype(jnp.bfloat16), w["w_down"])


def adamw(w, m, v, g):
    m = 0.9 * m + 0.1 * g
    v = 0.95 * v + 0.05 * g * g
    step = m * lax.rsqrt(v + 1e-8) + 0.1 * w
    return (w - 0.02 * step).astype(jnp.bfloat16), m, v


def stack(weights, h):
    return lax.scan(lambda h, w: (layer(h, w), None), h, weights)[0]


def reference(x, dy, w_gate, w_up, w_down, m_w_gate, m_w_up, m_w_down, v_w_gate, v_w_up, v_w_down):
    weights = dict(zip(NAMES, (w_gate, w_up, w_down), strict=True))

    def take(so_far, sequence):
        h, by_y = sequence
        _, back = jax.vjp(lambda w: stack(w, h), weights)
        return jax.tree.map(lambda total, term: total + term.astype(jnp.float32), so_far, back(by_y)[0]), None

    none_yet = {name: jnp.zeros(w.shape, jnp.float32) for name, w in weights.items()}
    by_weights, _ = lax.scan(take, none_yet, (x, dy))
    gradients = [by_weights[name].astype(jnp.bfloat16).astype(jnp.float32) for name in NAMES]
    new = [
        adamw(w.astype(jnp.float32), m, v, g)
        for w, m, v, g in zip((w_gate, w_up, w_down), (m_w_gate, m_w_up, m_w_down), (v_w_gate, v_w_up, v_w_down), gradients, strict=True)
    ]
    return tuple(one[which] for which in range(3) for one in new)
```

```python
import jax
import jax.numpy as jnp
from jax import lax
from jax.experimental import pallas as pl
from jax.experimental.pallas import tpu as pltpu
from jax.sharding import PartitionSpec as P

NAMES = ("w_gate", "w_up", "w_down")
F32, BF16 = jnp.float32, jnp.bfloat16
TN = 256
ANY = pl.BlockSpec(memory_space=pl.ANY)
NT = (((1,), (1,)), ((), ()))


def dot(a, b):
    return jnp.dot(a, b, preferred_element_type=F32)


def around():
    me = lax.axis_index("dp")

    def flip(i, bit):
        return i + bit - 2 * bit * ((i // bit) % 2)

    return me, flip


def rms(h):
    wide = h.astype(F32)
    return (wide * lax.rsqrt(jnp.mean(wide * wide, -1, keepdims=True) + 1e-6)).astype(BF16)


class Piece:
    def __init__(self, shard, full, layer, rows, columns=None):
        self.shard, self.full, self.layer, self.rows, self.columns = shard, full, layer, rows, columns

    def cut(self, part):
        if self.columns is None:
            n = self.rows if part is None else self.rows // 2
            return (n if part else 0), n, slice(None)
        at, width = self.columns
        n = width if part is None else width // 2
        return 0, self.rows, pl.ds(at + (n if part else 0), n)

    def own(self):
        off, n, cols = self.cut(None)
        return self.shard.at[self.layer, pl.ds(off, n), cols]

    def there(self, owner, part=None):
        off, n, cols = self.cut(part)
        return self.full.at[self.layer, pl.ds(pl.multiple_of(owner * self.rows + off, 16), n), cols]


def forward_kernel(units, tokens, d, ff, x, dy, wg, wu, wd, WG, WU, WD, gate0, up0, p0, h1, a0T, a1T, p1, dg1, du1,
                   a_vm, dy_vm, wd_vm, own_g, own_u, own_d, send, recv, local):
    me, flip = around()
    xn, yn, pn = flip(me, 4), flip(me, 2), flip(me, 1)
    diag = flip(xn, 2)
    rg, rd = wg.shape[1], wd.shape[1]

    barrier = pltpu.get_barrier_semaphore()
    for other in (xn, yn, pn):
        pl.semaphore_signal(barrier, inc=1, device_id={"dp": other}, device_id_type=pl.DeviceIdType.MESH)
    pl.semaphore_wait(barrier, 3)

    pieces, of_unit = [], []
    for what, layer, at, width in units:
        mine = []
        if what == "g":
            mine = [Piece(wg, WG, layer, rg, (at, width)), Piece(wu, WU, layer, rg, (at, width))]
        else:
            mine = [Piece(wd, WD, layer, rd)]
        of_unit.append(range(len(pieces), len(pieces) + len(mine)))
        pieces += mine

    def go(i, kind):
        piece = pieces[i]
        src, dst, to = {
            0: (None, (me, None), xn),
            1: (None, (me, None), yn),
            2: (None, (me, None), pn),
            3: ((xn, 1), (xn, 1), yn),
            4: ((yn, 0), (yn, 0), xn),
            5: ((xn, None), (xn, None), pn),
            6: ((yn, None), (yn, None), pn),
            7: ((diag, 0), (diag, 0), pn),
            8: ((diag, 1), (diag, 1), pn),
        }[kind]
        return pltpu.make_async_remote_copy(
            src_ref=piece.own() if src is None else piece.there(*src), dst_ref=piece.there(*dst),
            send_sem=send.at[i, kind], recv_sem=recv.at[i, kind],
            device_id={"dp": to}, device_id_type=pl.DeviceIdType.MESH)

    def come(i, kind):
        owner, part, sender = {
            0: (xn, None, xn), 1: (yn, None, yn), 2: (pn, None, pn), 3: (diag, 1, yn), 4: (diag, 0, xn),
            5: (flip(pn, 4), None, pn), 6: (flip(pn, 2), None, pn), 7: (flip(diag, 1), 0, pn), 8: (flip(diag, 1), 1, pn),
        }[kind]
        ref = pieces[i].there(owner, part)
        pltpu.make_async_remote_copy(
            src_ref=ref, dst_ref=ref, send_sem=send.at[i, kind], recv_sem=recv.at[i, kind],
            device_id={"dp": sender}, device_id_type=pl.DeviceIdType.MESH).wait_recv()

    def first(u):
        for i in of_unit[u] if u < len(units) else ():
            for kind in (0, 1, 2):
                go(i, kind).start()

    def relay(u):
        for i in of_unit[u]:
            come(i, 0)
            go(i, 3).start()
            go(i, 5).start()
            come(i, 1)
            go(i, 4).start()
            go(i, 6).start()
        first(u + 2)

    def last(u):
        for i in of_unit[u]:
            come(i, 4)
            go(i, 7).start()
            come(i, 3)
            go(i, 8).start()

    def complete(u):
        for i in of_unit[u]:
            for kind in (2, 5, 6, 7, 8):
                come(i, kind)

    first(0)
    first(1)
    load = [pltpu.make_async_copy(s, t, local.at[k]) for k, (s, t) in enumerate(((x, a_vm), (dy, dy_vm), (wg, own_g), (wu, own_u), (wd, own_d)))]
    for c in load:
        c.start()
    load[0].wait()

    @pl.loop(0, tokens // TN)
    def _(i):
        rows = pl.ds(pl.multiple_of(i * TN, TN), TN)
        a_vm[rows, :] = rms(a_vm[rows, :])

    for c in load[1:]:
        c.wait()
    stores = []
    for k, (own, full, rows) in enumerate(((own_g, WG, rg), (own_u, WU, rg), (own_d, WD, rd))):
        c = pltpu.make_async_copy(own, full.at[:, pl.ds(pl.multiple_of(me * rows, 16), rows), :], local.at[5 + k])
        c.start()
        stores.append(c)

    def transpose_out(j, out):
        out[...] = a_vm[pl.ds(pl.multiple_of(j * TN, TN), TN), :].T

    def transposed(aT):
        def body(idx, out):
            transpose_out(idx.index[0], out)
        pltpu.emit_pipeline(body, grid=(tokens // TN,), out_specs=[pl.BlockSpec((d, TN), lambda j: (0, j))], _explicit_indices=True)(aT)

    TM = 512

    def gate_up(at, width):
        def body(wg_t, wu_t, gate_t, up_t, p_t):
            @pl.loop(0, tokens // TM)
            def _(i):
                rows = pl.ds(pl.multiple_of(i * TM, TM), TM)
                a = a_vm[rows, :]
                g = dot(a, wg_t[...])
                u = dot(a, wu_t[...])
                gate_t[rows, :] = g
                up_t[rows, :] = u
                p_t[rows, :] = (g * jax.nn.sigmoid(g) * u).astype(BF16)
        j0 = at // TN
        w = pl.BlockSpec((d, TN), lambda j: (0, j + j0))
        o = pl.BlockSpec((tokens, TN), lambda j: (0, j + j0))
        pltpu.emit_pipeline(body, grid=(width // TN,), in_specs=[w, w], out_specs=[o, o, o])(WG.at[0], WU.at[0], gate0, up0, p0)

    def down():
        c = pltpu.make_async_copy(WD.at[0], wd_vm, local.at[8])
        c.start()
        c.wait()

        def body(idx, p_t, x_t, h_t):
            y = dot(p_t[...], wd_vm[...]).astype(BF16)
            h = x_t[...] + y
            h_t[...] = h
            a_vm[pl.ds(pl.multiple_of(idx.index[0] * TM, TM), TM), :] = rms(h)
        o = pl.BlockSpec((TM, d), lambda i: (i, 0))
        pltpu.emit_pipeline(body, grid=(tokens // TM,), in_specs=[pl.BlockSpec((TM, ff), lambda i: (i, 0)), o], out_specs=[o], _explicit_indices=True)(p0, x, h1)

    def gate_up_back(at, width):
        def body(wg_t, wu_t, wd_t, p_t, dg_t, du_t):
            @pl.loop(0, tokens // TM)
            def _(i):
                rows = pl.ds(pl.multiple_of(i * TM, TM), TM)
                a = a_vm[rows, :]
                g = dot(a, wg_t[...])
                u = dot(a, wu_t[...])
                dp = lax.dot_general(dy_vm[rows, :], wd_t[...], NT, preferred_element_type=F32).astype(BF16).astype(F32)
                sig = jax.nn.sigmoid(g)
                s = g * sig
                p_t[rows, :] = (s * u).astype(BF16)
                du_t[rows, :] = (dp * s).astype(BF16)
                dg_t[rows, :] = (dp * u * (sig + s * (1 - sig))).astype(BF16)
        j0 = at // TN
        w = pl.BlockSpec((d, TN), lambda j: (0, j + j0))
        o = pl.BlockSpec((tokens, TN), lambda j: (0, j + j0))
        pltpu.emit_pipeline(body, grid=(width // TN,), in_specs=[w, w, pl.BlockSpec((TN, d), lambda j: (j + j0, 0))], out_specs=[o, o, o])(
            WG.at[1], WU.at[1], WD.at[1], p1, dg1, du1)

    transposed(a0T)
    for c in stores:
        c.wait()
    relay(0)
    n = len(units)
    for u, (what, layer, at, width) in enumerate(units):
        if u + 1 < n:
            relay(u + 1)
        last(u)
        complete(u)
        if what == "g" and layer == 0:
            gate_up(at, width)
        elif what == "g":
            gate_up_back(at, width)
        elif layer == 0:
            down()
            transposed(a1T)
    for i in range(len(pieces)):
        for kind in range(9):
            go(i, kind).wait_send()


def forward(x, dy, wg, wu, wd):
    tokens, d = x.shape
    ff = wg.shape[2]
    tiles = ff // TN
    a, b = (tiles + 1) // 2 * TN, tiles // 2 * TN
    units = [("g", 0, 0, a), ("g", 0, a, b), ("d", 0, 0, 0), ("d", 1, 0, 0)]
    at = 0
    for k in range(4):
        w = (tiles + 3 - k) // 4 * TN
        units.append(("g", 1, at, w))
        at += w
    assert at == ff
    count = sum(2 if u[0] == "g" else 1 for u in units)
    big = jax.ShapeDtypeStruct((tokens, ff), BF16)
    wide = jax.ShapeDtypeStruct((tokens, ff), F32)
    h = jax.ShapeDtypeStruct((tokens, d), BF16)
    hT = jax.ShapeDtypeStruct((d, tokens), BF16)
    outs = [jax.ShapeDtypeStruct((2, d, ff), BF16)] * 2 + [jax.ShapeDtypeStruct((2, ff, d), BF16), wide, wide, big, h, hT, hT, big, big, big]

    def kernel(*refs):
        forward_kernel(units, tokens, d, ff, *refs)

    return pl.pallas_call(
        kernel,
        out_shape=outs,
        in_specs=[ANY] * 5,
        out_specs=[ANY] * len(outs),
        scratch_shapes=[
            pltpu.VMEM((tokens, d), BF16), pltpu.VMEM((tokens, d), BF16), pltpu.VMEM((ff, d), BF16),
            pltpu.VMEM(wg.shape, BF16), pltpu.VMEM(wu.shape, BF16), pltpu.VMEM(wd.shape, BF16),
            pltpu.SemaphoreType.DMA((count, 9)), pltpu.SemaphoreType.DMA((count, 9)), pltpu.SemaphoreType.DMA((9,)),
        ],
        compiler_params=pltpu.CompilerParams(collective_id=0, has_side_effects=True, vmem_limit_bytes=60 * 2**20),
        name="forward",
    )(x, dy, wg, wu, wd)


def adamw(w, m, v, g):
    m = 0.9 * m + 0.1 * g
    v = 0.95 * v + 0.05 * g * g
    step = m * lax.rsqrt(v + 1e-8) + 0.1 * w
    return (w - 0.02 * step).astype(BF16), m, v


def scatter(g):
    return lax.psum_scatter(g.astype(BF16), "dp", scatter_dimension=0, tiled=True)


def solution(mesh):
    def step(x, dy, *arrays):
        weights, m, v = (arrays[i : i + 3] for i in (0, 3, 6))
        x, dy = x[0], dy[0]
        WG, WU, WD, gate0, up0, p0, h1, a0T, a1T, p1, dg1, du1 = forward(x, dy, *weights)
        d1 = [scatter(dot(a1T, dg1)), scatter(dot(a1T, du1)), scatter(dot(p1.T, dy))]
        da = lax.dot_general(dg1, WG[1], NT, preferred_element_type=F32).astype(BF16) + lax.dot_general(du1, WU[1], NT, preferred_element_type=F32).astype(BF16)
        wide, da = h1.astype(F32), da.astype(F32)
        scale = lax.rsqrt(jnp.mean(wide * wide, -1, keepdims=True) + 1e-6)
        dh = dy + (scale * (da - wide * (scale * scale * jnp.mean(da * wide, -1, keepdims=True)))).astype(BF16)
        dp = lax.dot_general(dh, WD[0], NT, preferred_element_type=F32).astype(BF16).astype(F32)
        sig = jax.nn.sigmoid(gate0)
        s = gate0 * sig
        du0 = (dp * s).astype(BF16)
        dg0 = (dp * up0 * (sig + s * (1 - sig))).astype(BF16)
        d0 = [scatter(dot(a0T, dg0)), scatter(dot(a0T, du0)), scatter(dot(p0.T, dh))]
        gradients = [jnp.stack([d0[i], d1[i]]).astype(F32) for i in range(3)]
        new = [adamw(w.astype(F32), m, v, g) for w, m, v, g in zip(weights, m, v, gradients, strict=True)]
        return tuple(one[which] for which in range(3) for one in new)

    states, cut = P(("rep", "dp"), None, None), P(None, "dp", None)
    return jax.shard_map(
        step,
        mesh=mesh,
        in_specs=(states, states) + (cut,) * 9,
        out_specs=(P("rep", "dp", None),) * 9,
        check_vma=False,
    )
```

```python
import jax
import jax.numpy as jnp
from jax import lax
from jax.experimental import pallas as pl
from jax.experimental.pallas import tpu as pltpu
from jax.sharding import PartitionSpec as P

NAMES = ("w_gate", "w_up", "w_down")
F32, BF16 = jnp.float32, jnp.bfloat16
TN = 256
ANY = pl.BlockSpec(memory_space=pl.ANY)
NT = (((1,), (1,)), ((), ()))


def dot(a, b):
    return jnp.dot(a, b, preferred_element_type=F32)


def around():
    me = lax.axis_index("dp")

    def flip(i, bit):
        return i + bit - 2 * bit * ((i // bit) % 2)

    return me, flip


def rms(h):
    wide = h.astype(F32)
    return (wide * lax.rsqrt(jnp.mean(wide * wide, -1, keepdims=True) + 1e-6)).astype(BF16)


class Piece:
    def __init__(self, shard, full, layer, rows, columns=None):
        self.shard, self.full, self.layer, self.rows, self.columns = shard, full, layer, rows, columns

    def cut(self, part):
        if self.columns is None:
            n = self.rows if part is None else self.rows // 2
            return (n if part else 0), n, slice(None)
        at, width = self.columns
        n = width if part is None else width // 2
        return 0, self.rows, pl.ds(at + (n if part else 0), n)

    def own(self):
        off, n, cols = self.cut(None)
        return self.shard.at[self.layer, pl.ds(off, n), cols]

    def there(self, owner, part=None):
        off, n, cols = self.cut(part)
        return self.full.at[self.layer, pl.ds(pl.multiple_of(owner * self.rows + off, 16), n), cols]


def forward_kernel(units, tokens, d, ff, x, dy, wg, wu, wd, WG, WU, WD, gate0, up0, p0, h1, a0T, a1T, p1, dg1, du1,
                   a_vm, dy_vm, wd_vm, own_g, own_u, own_d, send, recv, local):
    me, flip = around()
    xn, yn, pn = flip(me, 4), flip(me, 2), flip(me, 1)
    diag = flip(xn, 2)
    rg, rd = wg.shape[1], wd.shape[1]

    barrier = pltpu.get_barrier_semaphore()
    for other in (xn, yn, pn):
        pl.semaphore_signal(barrier, inc=1, device_id={"dp": other}, device_id_type=pl.DeviceIdType.MESH)
    pl.semaphore_wait(barrier, 3)

    pieces, of_unit = [], []
    for what, layer, at, width in units:
        mine = []
        if what == "g":
            mine = [Piece(wg, WG, layer, rg, (at, width)), Piece(wu, WU, layer, rg, (at, width))]
        else:
            mine = [Piece(wd, WD, layer, rd)]
        of_unit.append(range(len(pieces), len(pieces) + len(mine)))
        pieces += mine

    def go(i, kind):
        piece = pieces[i]
        src, dst, to = {
            0: (None, (me, None), xn),
            1: (None, (me, None), yn),
            2: (None, (me, None), pn),
            3: ((xn, 1), (xn, 1), yn),
            4: ((yn, 0), (yn, 0), xn),
            5: ((xn, None), (xn, None), pn),
            6: ((yn, None), (yn, None), pn),
            7: ((diag, 0), (diag, 0), pn),
            8: ((diag, 1), (diag, 1), pn),
        }[kind]
        return pltpu.make_async_remote_copy(
            src_ref=piece.own() if src is None else piece.there(*src), dst_ref=piece.there(*dst),
            send_sem=send.at[i, kind], recv_sem=recv.at[i, kind],
            device_id={"dp": to}, device_id_type=pl.DeviceIdType.MESH)

    def come(i, kind):
        owner, part, sender = {
            0: (xn, None, xn), 1: (yn, None, yn), 2: (pn, None, pn), 3: (diag, 1, yn), 4: (diag, 0, xn),
            5: (flip(pn, 4), None, pn), 6: (flip(pn, 2), None, pn), 7: (flip(diag, 1), 0, pn), 8: (flip(diag, 1), 1, pn),
        }[kind]
        ref = pieces[i].there(owner, part)
        pltpu.make_async_remote_copy(
            src_ref=ref, dst_ref=ref, send_sem=send.at[i, kind], recv_sem=recv.at[i, kind],
            device_id={"dp": sender}, device_id_type=pl.DeviceIdType.MESH).wait_recv()

    def first(u):
        for i in of_unit[u] if u < len(units) else ():
            for kind in (0, 1, 2):
                go(i, kind).start()

    def relay(u):
        for i in of_unit[u]:
            come(i, 0)
            go(i, 3).start()
            go(i, 5).start()
            come(i, 1)
            go(i, 4).start()
            go(i, 6).start()
        first(u + 2)

    def last(u):
        for i in of_unit[u]:
            come(i, 4)
            go(i, 7).start()
            come(i, 3)
            go(i, 8).start()

    def complete(u):
        for i in of_unit[u]:
            for kind in (2, 5, 6, 7, 8):
                come(i, kind)

    first(0)
    first(1)
    load = [pltpu.make_async_copy(s, t, local.at[k]) for k, (s, t) in enumerate(((x, a_vm), (dy, dy_vm), (wg, own_g), (wu, own_u), (wd, own_d)))]
    for c in load:
        c.start()
    load[0].wait()

    @pl.loop(0, tokens // TN)
    def _(i):
        rows = pl.ds(pl.multiple_of(i * TN, TN), TN)
        a_vm[rows, :] = rms(a_vm[rows, :])

    for c in load[1:]:
        c.wait()
    stores = []
    for k, (own, full, rows) in enumerate(((own_g, WG, rg), (own_u, WU, rg), (own_d, WD, rd))):
        c = pltpu.make_async_copy(own, full.at[:, pl.ds(pl.multiple_of(me * rows, 16), rows), :], local.at[5 + k])
        c.start()
        stores.append(c)

    def transpose_out(j, out):
        out[...] = a_vm[pl.ds(pl.multiple_of(j * TN, TN), TN), :].T

    def transposed(aT):
        def body(idx, out):
            transpose_out(idx.index[0], out)
        pltpu.emit_pipeline(body, grid=(tokens // TN,), out_specs=[pl.BlockSpec((d, TN), lambda j: (0, j))], _explicit_indices=True)(aT)

    TM = 512

    def gate_up(at, width):
        def body(wg_t, wu_t, gate_t, up_t, p_t):
            @pl.loop(0, tokens // TM)
            def _(i):
                rows = pl.ds(pl.multiple_of(i * TM, TM), TM)
                a = a_vm[rows, :]
                g = dot(a, wg_t[...])
                u = dot(a, wu_t[...])
                gate_t[rows, :] = g
                up_t[rows, :] = u
                p_t[rows, :] = (g * jax.nn.sigmoid(g) * u).astype(BF16)
        j0 = at // TN
        w = pl.BlockSpec((d, TN), lambda j: (0, j + j0))
        o = pl.BlockSpec((tokens, TN), lambda j: (0, j + j0))
        pltpu.emit_pipeline(body, grid=(width // TN,), in_specs=[w, w], out_specs=[o, o, o])(WG.at[0], WU.at[0], gate0, up0, p0)

    def down():
        c = pltpu.make_async_copy(WD.at[0], wd_vm, local.at[8])
        c.start()
        c.wait()

        def body(idx, p_t, x_t, h_t):
            y = dot(p_t[...], wd_vm[...]).astype(BF16)
            h = x_t[...] + y
            h_t[...] = h
            a_vm[pl.ds(pl.multiple_of(idx.index[0] * TM, TM), TM), :] = rms(h)
        o = pl.BlockSpec((TM, d), lambda i: (i, 0))
        pltpu.emit_pipeline(body, grid=(tokens // TM,), in_specs=[pl.BlockSpec((TM, ff), lambda i: (i, 0)), o], out_specs=[o], _explicit_indices=True)(p0, x, h1)

    def gate_up_back(at, width):
        def body(wg_t, wu_t, wd_t, p_t, dg_t, du_t):
            @pl.loop(0, tokens // TM)
            def _(i):
                rows = pl.ds(pl.multiple_of(i * TM, TM), TM)
                a = a_vm[rows, :]
                g = dot(a, wg_t[...])
                u = dot(a, wu_t[...])
                dp = lax.dot_general(dy_vm[rows, :], wd_t[...], NT, preferred_element_type=F32).astype(BF16).astype(F32)
                sig = jax.nn.sigmoid(g)
                s = g * sig
                p_t[rows, :] = (s * u).astype(BF16)
                du_t[rows, :] = (dp * s).astype(BF16)
                dg_t[rows, :] = (dp * u * (sig + s * (1 - sig))).astype(BF16)
        j0 = at // TN
        w = pl.BlockSpec((d, TN), lambda j: (0, j + j0))
        o = pl.BlockSpec((tokens, TN), lambda j: (0, j + j0))
        pltpu.emit_pipeline(body, grid=(width // TN,), in_specs=[w, w, pl.BlockSpec((TN, d), lambda j: (j + j0, 0))], out_specs=[o, o, o])(
            WG.at[1], WU.at[1], WD.at[1], p1, dg1, du1)

    transposed(a0T)
    for c in stores:
        c.wait()
    relay(0)
    n = len(units)
    for u, (what, layer, at, width) in enumerate(units):
        if u + 1 < n:
            relay(u + 1)
        last(u)
        complete(u)
        if what == "g" and layer == 0:
            gate_up(at, width)
        elif what == "g":
            gate_up_back(at, width)
        elif layer == 0:
            down()
            transposed(a1T)
    for i in range(len(pieces)):
        for kind in range(9):
            go(i, kind).wait_send()


def forward(x, dy, wg, wu, wd):
    tokens, d = x.shape
    ff = wg.shape[2]
    tiles = ff // TN
    a, b = (tiles + 1) // 2 * TN, tiles // 2 * TN
    units = [("g", 0, 0, a), ("g", 0, a, b), ("d", 0, 0, 0), ("d", 1, 0, 0)]
    at = 0
    for k in range(4):
        w = (tiles + 3 - k) // 4 * TN
        units.append(("g", 1, at, w))
        at += w
    assert at == ff
    count = sum(2 if u[0] == "g" else 1 for u in units)
    big = jax.ShapeDtypeStruct((tokens, ff), BF16)
    wide = jax.ShapeDtypeStruct((tokens, ff), F32)
    h = jax.ShapeDtypeStruct((tokens, d), BF16)
    hT = jax.ShapeDtypeStruct((d, tokens), BF16)
    outs = [jax.ShapeDtypeStruct((2, d, ff), BF16)] * 2 + [jax.ShapeDtypeStruct((2, ff, d), BF16), wide, wide, big, h, hT, hT, big, big, big]

    def kernel(*refs):
        forward_kernel(units, tokens, d, ff, *refs)

    return pl.pallas_call(
        kernel,
        out_shape=outs,
        in_specs=[ANY] * 5,
        out_specs=[ANY] * len(outs),
        scratch_shapes=[
            pltpu.VMEM((tokens, d), BF16), pltpu.VMEM((tokens, d), BF16), pltpu.VMEM((ff, d), BF16),
            pltpu.VMEM(wg.shape, BF16), pltpu.VMEM(wu.shape, BF16), pltpu.VMEM(wd.shape, BF16),
            pltpu.SemaphoreType.DMA((count, 9)), pltpu.SemaphoreType.DMA((count, 9)), pltpu.SemaphoreType.DMA((9,)),
        ],
        compiler_params=pltpu.CompilerParams(collective_id=0, has_side_effects=True, vmem_limit_bytes=60 * 2**20),
        name="forward",
    )(x, dy, wg, wu, wd)


class Unit:
    def __init__(self, n, slot, bufs, rows, width, by_rows, outs, older, newer):
        self.n, self.slot, self.rows, self.width, self.by_rows, self.outs, self.older, self.newer = n, slot, rows, width, by_rows, outs, older, newer
        self.G, self.Rp, self.R1, self.R2 = bufs
        self.pieces = len(outs)
        self.h = (rows if by_rows else width) // 2

    def block(self, b):
        return self.G.at[:, pl.ds(pl.multiple_of(b * self.rows, 16), self.rows), pl.ds(0, self.width)]

    def half(self, b, part):
        if self.by_rows:
            return self.G.at[:, pl.ds(pl.multiple_of(b * self.rows + part * self.h, 16), self.h), :]
        return self.G.at[:, pl.ds(pl.multiple_of(b * self.rows, 16), self.rows), pl.ds(part * self.h, self.h)]

    def narrow(self, ref):
        return ref if self.by_rows else ref.at[:, :, pl.ds(0, self.h)]

    def r1(self, part, which):
        return self.narrow(self.R1.at[part, which])

    def r2(self, part):
        return self.narrow(self.R2.at[part])

    def rp(self, q):
        return self.Rp.at[q, :, :, pl.ds(0, self.width)]


def backward_kernel(groups, tokens, d, ff, p1, dg1, du1, a1T, dy, WG, WU, WD, h1, gate0, up0, p0, a0T, gG, gU, gD,
                    aT_vm, dh_vm, Gg, Rpg, R1g, R2g, Gd, Rpd, R1d, R2d, send, recv, local, credit):
    me, flip = around()
    xn, yn, pn = flip(me, 4), flip(me, 2), flip(me, 1)
    core, q0 = me % 2, me // 2
    qx, qy = flip(q0, 2), flip(q0, 1)
    qd = flip(qx, 1)
    rg, rd = d // 8, ff // 8
    SLOTS = Gg.shape[0]

    barrier = pltpu.get_barrier_semaphore()
    for other in (xn, yn, pn):
        pl.semaphore_signal(barrier, inc=1, device_id={"dp": other}, device_id_type=pl.DeviceIdType.MESH)
    pl.semaphore_wait(barrier, 3)

    down_bufs = (Gd, Rpd, R1d, R2d)
    count = len(groups)
    D = [Unit(2 * count + 1, SLOTS, down_bufs, rd, d, True, [gD.at[0]], True, False),
         Unit(2 * count, SLOTS, down_bufs, rd, d, True, [gD.at[1]], False, True)]
    units = []
    for layer in (1, 0):
        for at, width in groups:
            n = len(units)
            s = n % SLOTS
            cols = pl.ds(at, width)
            units.append(Unit(n, s, (Gg.at[s], Rpg.at[s], R1g.at[s], R2g.at[s]), rg, width, False,
                              [gG.at[layer, :, cols], gU.at[layer, :, cols]], n >= SLOTS, n + SLOTS < 2 * count))

    def remote(u, k, src, dst, to):
        return pltpu.make_async_remote_copy(src_ref=src, dst_ref=dst, send_sem=send.at[u.n, k], recv_sem=recv.at[u.n, k],
                                            device_id={"dp": to}, device_id_type=pl.DeviceIdType.MESH)

    def to_partner(u, q):
        return remote(u, q, u.block(2 * q + 1 - core), u.rp(q), pn)

    def stage1(u, k):
        q, part, which, to = ((qd, 0, 1, xn), (qd, 1, 1, yn), (qx, 0, 0, xn), (qy, 1, 0, yn))[k]
        return remote(u, 4 + k, u.half(2 * q + core, part), u.r1(part, which), to)

    def stage2(u, k):
        q, to = ((qy, yn), (qx, xn))[k]
        return remote(u, 8 + k, u.half(2 * q + core, k), u.r2(k), to)

    def grant(u, k, to):
        pl.semaphore_signal(credit.at[u.slot, k], inc=1, device_id={"dp": to}, device_id_type=pl.DeviceIdType.MESH)

    def add(dst, *others):
        for i in range(dst.shape[0]):
            total = dst[i].astype(F32)
            for other in others:
                total = total + other[i].astype(F32)
            dst[i] = total.astype(BF16)

    def s0(u):
        if u.older:
            pl.semaphore_wait(credit.at[u.slot, 0], 1)
        for q in range(4):
            to_partner(u, q).start()

    def s1(u):
        for q in range(4):
            to_partner(u, q).wait_recv()

        @pl.loop(0, 4)
        def _(q):
            add(u.block(2 * q + core), u.rp(q))
        if u.newer:
            grant(u, 0, pn)
        if u.older:
            pl.semaphore_wait(credit.at[u.slot, 1], 1)
            pl.semaphore_wait(credit.at[u.slot, 2], 1)
        for k in range(4):
            stage1(u, k).start()

    def s2(u):
        stage1(u, 0).wait_recv()
        add(u.half(2 * qy + core, 0), u.r1(0, 1))
        stage2(u, 0).start()
        stage1(u, 1).wait_recv()
        add(u.half(2 * qx + core, 1), u.r1(1, 1))
        stage2(u, 1).start()

    def out(u, i):
        return pltpu.make_async_copy(u.block(me).at[i], u.outs[i], local.at[u.n, i])

    def s3(u):
        for k in (2, 3):
            stage1(u, k).wait_recv()
        for part in (0, 1):
            stage2(u, part).wait_recv()
            add(u.half(me, part), u.r1(part, 0), u.r2(part))
        for i in range(u.pieces):
            out(u, i).start()
        if u.newer:
            grant(u, 1, xn)
            grant(u, 2, yn)
        for q in range(4):
            to_partner(u, q).wait_send()
        for k in range(4):
            stage1(u, k).wait_send()
        for k in range(2):
            stage2(u, k).wait_send()

    def s4(u):
        for i in range(u.pieces):
            out(u, i).wait()

    def run(events, j):
        for at in sorted({e[0] for e in events}):
            @pl.when(j == at)
            def _(at=at):
                for when, what, u in events:
                    if when == at:
                        what(u)

    TM = 512
    wide_tile = pl.BlockSpec((tokens, TN), lambda j: (0, j))
    w_tile = pl.BlockSpec((d, TN), lambda j: (0, j))

    def load(src, dst):
        c = pltpu.make_async_copy(src, dst, local.at[0, 0])
        c.start()
        c.wait()

    def down_weight(p, unit, events):
        def body(idx, p_t):
            j = idx.index[0]
            run(events, j)
            g = lax.dot_general(p_t[...], dh_vm[...], (((0,), (0,)), ((), ())), preferred_element_type=F32)
            unit.G[0, pl.ds(pl.multiple_of(j * TN, TN), TN), :] = g.astype(BF16)
        pltpu.emit_pipeline(body, grid=(ff // TN,), in_specs=[wide_tile], _explicit_indices=True)(p)

    def store_weight(mine, j, i, g_t):
        value = dot(aT_vm[...], g_t[...]).astype(BF16)
        for k, u in enumerate(mine):
            at, width = groups[k]

            @pl.when((j >= at // TN) & (j < (at + width) // TN))
            def _(u=u, at=at):
                u.G[i, :, pl.ds(pl.multiple_of(j * TN - at, TN), TN)] = value

    def layer1(acc, events):
        mine = units[:count]

        def body(idx, dg_t, du_t, wg_t, wu_t):
            j = idx.index[0]
            run(events, j)
            store_weight(mine, j, 0, dg_t)
            store_weight(mine, j, 1, du_t)

            def both(i):
                rows = pl.ds(pl.multiple_of(i * TM, TM), TM)
                return rows, lax.dot_general(dg_t[rows, :], wg_t[...], NT, preferred_element_type=F32) + lax.dot_general(
                    du_t[rows, :], wu_t[...], NT, preferred_element_type=F32)

            @pl.loop(0, tokens // TM)
            def _(i):
                rows, value = both(i)
                acc[rows, :] = jnp.where(j == 0, value, acc[rows, :] + value)
        pltpu.emit_pipeline(body, grid=(ff // TN,), in_specs=[wide_tile, wide_tile, w_tile, w_tile], _explicit_indices=True)(dg1, du1, WG.at[1], WU.at[1])

        def norm(idx, h_t):
            rows = pl.ds(pl.multiple_of(idx.index[0] * TN, TN), TN)
            wide = h_t[...].astype(F32)
            da = acc[rows, :].astype(BF16).astype(F32)
            scale = lax.rsqrt(jnp.mean(wide * wide, -1, keepdims=True) + 1e-6)
            back = scale * (da - wide * (scale * scale * jnp.mean(da * wide, -1, keepdims=True)))
            dh_vm[rows, :] = dh_vm[rows, :] + back.astype(BF16)
        pltpu.emit_pipeline(norm, grid=(tokens // TN,), in_specs=[pl.BlockSpec((TN, d), lambda i: (i, 0))], _explicit_indices=True)(h1)

    def layer0(dg_vm, du_vm, events):
        mine = units[count:]

        def body(idx, wd_t, gate_t, up_t):
            j = idx.index[0]
            run(events, j)

            @pl.loop(0, tokens // TM)
            def _(i):
                rows = pl.ds(pl.multiple_of(i * TM, TM), TM)
                dp = lax.dot_general(dh_vm[rows, :], wd_t[...], NT, preferred_element_type=F32).astype(BF16).astype(F32)
                g = gate_t[rows, :]
                sig = jax.nn.sigmoid(g)
                s = g * sig
                du_vm[rows, :] = (dp * s).astype(BF16)
                dg_vm[rows, :] = (dp * up_t[rows, :] * (sig + s * (1 - sig))).astype(BF16)
            store_weight(mine, j, 0, dg_vm)
            store_weight(mine, j, 1, du_vm)
        pltpu.emit_pipeline(body, grid=(ff // TN,), in_specs=[pl.BlockSpec((TN, d), lambda j: (j, 0)), wide_tile, wide_tile], _explicit_indices=True)(
            WD.at[0], gate0, up0)

    tiles = ff // TN
    order = {"D1": [], "L1": [], "D0": [], "L0": [], "end": []}

    def spot(tick):
        if tick < tiles:
            return "L1", tick
        tick -= tiles
        if tick < 5:
            return "D0", 4 * tick
        tick -= 5
        return ("L0", tick) if tick < tiles else ("end", tick)

    def plan(u, ticks):
        for tick, what in zip(ticks, (s0, s1, s2, s3, s4)):
            where, at = spot(tick)
            order[where].append((at, what, u))

    plan(D[1], (0, 2, 9, 12, 14))
    for k, u in enumerate(units):
        at, width = groups[k % count]
        end = (at + width) // TN + (0 if k < count else tiles + 5)
        plan(u, (end, end + 1, end + 5, end + 7, end + 8))
    start = tiles + 5
    plan(D[0], (start, start + 2, start + 9, start + 12, start + 14))
    for events in order.values():
        events.sort(key=lambda e: (e[0], -(s0, s1, s2, s3, s4).index(e[1])))

    load(dy, dh_vm)
    load(a1T, aT_vm)
    down_weight(p1, D[1], [])
    pl.run_scoped(lambda acc: layer1(acc, order["L1"]), pltpu.VMEM((tokens, d), F32))
    load(a0T, aT_vm)
    down_weight(p0, D[0], order["D0"])
    pl.run_scoped(lambda a, b: layer0(a, b, order["L0"]), pltpu.VMEM((tokens, TN), BF16), pltpu.VMEM((tokens, TN), BF16))
    for _, what, u in order["end"]:
        what(u)


def backward(p1, dg1, du1, a1T, dy, WG, WU, WD, h1, gate0, up0, p0, a0T):
    tokens, d = dy.shape
    ff = dg1.shape[1]
    tiles, groups, at = ff // TN, [], 0
    while at < ff:
        width = min(4 * TN, ff - at)
        groups.append((at, width))
        at += width
    C, rg, rd, slots, n = 4 * TN, d // 8, ff // 8, 3, 2 * len(groups) + 2
    outs = [jax.ShapeDtypeStruct((2, rg, ff), BF16)] * 2 + [jax.ShapeDtypeStruct((2, rd, d), BF16)]

    def kernel(*refs):
        backward_kernel(groups, tokens, d, ff, *refs)

    return pl.pallas_call(
        kernel,
        out_shape=outs,
        in_specs=[ANY] * 13,
        out_specs=[ANY] * 3,
        scratch_shapes=[
            pltpu.VMEM((d, tokens), BF16), pltpu.VMEM((tokens, d), BF16),
            pltpu.VMEM((slots, 2, d, C), BF16), pltpu.VMEM((slots, 4, 2, rg, C), BF16),
            pltpu.VMEM((slots, 2, 2, 2, rg, C // 2), BF16), pltpu.VMEM((slots, 2, 2, rg, C // 2), BF16),
            pltpu.VMEM((1, ff, d), BF16), pltpu.VMEM((4, 1, rd, d), BF16),
            pltpu.VMEM((2, 2, 1, rd // 2, d), BF16), pltpu.VMEM((2, 1, rd // 2, d), BF16),
            pltpu.SemaphoreType.DMA((n, 10)), pltpu.SemaphoreType.DMA((n, 10)), pltpu.SemaphoreType.DMA((n, 2)),
            pltpu.SemaphoreType.REGULAR((slots + 1, 3)),
        ],
        compiler_params=pltpu.CompilerParams(collective_id=1, has_side_effects=True, vmem_limit_bytes=67000000),
        name="backward",
    )(p1, dg1, du1, a1T, dy, WG, WU, WD, h1, gate0, up0, p0, a0T)


def adamw(w, m, v, g):
    m = 0.9 * m + 0.1 * g
    v = 0.95 * v + 0.05 * g * g
    step = m * lax.rsqrt(v + 1e-8) + 0.1 * w
    return (w - 0.02 * step).astype(BF16), m, v


def solution(mesh):
    def step(x, dy, *arrays):
        weights, m, v = (arrays[i : i + 3] for i in (0, 3, 6))
        x, dy = x[0], dy[0]
        WG, WU, WD, gate0, up0, p0, h1, a0T, a1T, p1, dg1, du1 = forward(x, dy, *weights)
        gradients = [g.astype(F32) for g in backward(p1, dg1, du1, a1T, dy, WG, WU, WD, h1, gate0, up0, p0, a0T)]
        new = [adamw(w.astype(F32), m, v, g) for w, m, v, g in zip(weights, m, v, gradients, strict=True)]
        return tuple(one[which] for which in range(3) for one in new)

    states, cut = P(("rep", "dp"), None, None), P(None, "dp", None)
    return jax.shard_map(
        step,
        mesh=mesh,
        in_specs=(states, states) + (cut,) * 9,
        out_specs=(P("rep", "dp", None),) * 9,
        check_vma=False,
    )
```

```python
import jax
import jax.numpy as jnp
from jax import lax
from jax.experimental import pallas as pl
from jax.experimental.pallas import tpu as pltpu
from jax.sharding import PartitionSpec as P

NAMES = ("w_gate", "w_up", "w_down")
F32, BF16 = jnp.float32, jnp.bfloat16
TN = 256
GROUP = 3 * TN
ANY = pl.BlockSpec(memory_space=pl.ANY)
NT, TT = (((1,), (1,)), ((), ())), (((0,), (0,)), ((), ()))


def dot(a, b):
    return jnp.dot(a, b, preferred_element_type=F32)


def around():
    me = lax.axis_index("dp")

    def flip(i, bit):
        return i + bit - 2 * bit * ((i // bit) % 2)

    return me, flip


def rms(h):
    wide = h.astype(F32)
    return (wide * lax.rsqrt(jnp.mean(wide * wide, -1, keepdims=True) + 1e-6)).astype(BF16)


class Piece:
    def __init__(self, shard, full, layer, rows, columns=None):
        self.shard, self.full, self.layer, self.rows, self.columns = shard, full, layer, rows, columns

    def cut(self, part):
        if self.columns is None:
            n = self.rows if part is None else self.rows // 2
            return (n if part else 0), n, slice(None)
        at, width = self.columns
        n = width if part is None else width // 2
        return 0, self.rows, pl.ds(at + (n if part else 0), n)

    def own(self):
        off, n, cols = self.cut(None)
        return self.shard.at[self.layer, pl.ds(off, n), cols]

    def there(self, owner, part=None):
        off, n, cols = self.cut(part)
        return self.full.at[self.layer, pl.ds(pl.multiple_of(owner * self.rows + off, 16), n), cols]


def forward_kernel(units, tokens, d, ff, x, dy, wg, wu, wd, WG, WU, WD, f0, e0, p0, h1, a0T, a1T, gd1, dg1, du1,
                   a_vm, dy_vm, wd_vm, p_vm, own_g, own_u, own_d, send, recv, local):
    me, flip = around()
    xn, yn, pn = flip(me, 4), flip(me, 2), flip(me, 1)
    diag = flip(xn, 2)
    rg, rd = wg.shape[1], wd.shape[1]

    barrier = pltpu.get_barrier_semaphore()
    for other in (xn, yn, pn):
        pl.semaphore_signal(barrier, inc=1, device_id={"dp": other}, device_id_type=pl.DeviceIdType.MESH)
    pl.semaphore_wait(barrier, 3)

    pieces, of_unit = [], []
    for what, layer, at, width in units:
        mine = []
        if what == "g":
            mine = [Piece(wg, WG, layer, rg, (at, width)), Piece(wu, WU, layer, rg, (at, width))]
        else:
            mine = [Piece(wd, WD, layer, rd)]
        of_unit.append(range(len(pieces), len(pieces) + len(mine)))
        pieces += mine

    def go(i, kind):
        piece = pieces[i]
        src, dst, to = {
            0: (None, (me, None), xn),
            1: (None, (me, None), yn),
            2: (None, (me, None), pn),
            3: ((xn, 1), (xn, 1), yn),
            4: ((yn, 0), (yn, 0), xn),
            5: ((xn, None), (xn, None), pn),
            6: ((yn, None), (yn, None), pn),
            7: ((diag, 0), (diag, 0), pn),
            8: ((diag, 1), (diag, 1), pn),
        }[kind]
        return pltpu.make_async_remote_copy(
            src_ref=piece.own() if src is None else piece.there(*src), dst_ref=piece.there(*dst),
            send_sem=send.at[i, kind], recv_sem=recv.at[i, kind],
            device_id={"dp": to}, device_id_type=pl.DeviceIdType.MESH)

    def come(i, kind):
        owner, part, sender = {
            0: (xn, None, xn), 1: (yn, None, yn), 2: (pn, None, pn), 3: (diag, 1, yn), 4: (diag, 0, xn),
            5: (flip(pn, 4), None, pn), 6: (flip(pn, 2), None, pn), 7: (flip(diag, 1), 0, pn), 8: (flip(diag, 1), 1, pn),
        }[kind]
        ref = pieces[i].there(owner, part)
        pltpu.make_async_remote_copy(
            src_ref=ref, dst_ref=ref, send_sem=send.at[i, kind], recv_sem=recv.at[i, kind],
            device_id={"dp": sender}, device_id_type=pl.DeviceIdType.MESH).wait_recv()

    def first(u):
        for i in of_unit[u] if u < len(units) else ():
            for kind in (0, 1, 2):
                go(i, kind).start()

    def relay(u):
        for i in of_unit[u]:
            come(i, 0)
            go(i, 3).start()
            go(i, 5).start()
            come(i, 1)
            go(i, 4).start()
            go(i, 6).start()
        first(u + 2)

    def last(u):
        for i in of_unit[u]:
            come(i, 4)
            go(i, 7).start()
            come(i, 3)
            go(i, 8).start()

    def complete(u):
        for i in of_unit[u]:
            for kind in (2, 5, 6, 7, 8):
                come(i, kind)

    first(0)
    first(1)
    load = [pltpu.make_async_copy(s, t, local.at[k]) for k, (s, t) in enumerate(((x, a_vm), (dy, dy_vm), (wg, own_g), (wu, own_u), (wd, own_d)))]
    for c in load:
        c.start()
    load[0].wait()

    @pl.loop(0, tokens // TN)
    def _(i):
        rows = pl.ds(pl.multiple_of(i * TN, TN), TN)
        a_vm[rows, :] = rms(a_vm[rows, :])

    for c in load[1:]:
        c.wait()
    stores = []
    for k, (own, full, rows) in enumerate(((own_g, WG, rg), (own_u, WU, rg), (own_d, WD, rd))):
        c = pltpu.make_async_copy(own, full.at[:, pl.ds(pl.multiple_of(me * rows, 16), rows), :], local.at[5 + k])
        c.start()
        stores.append(c)

    def transpose_out(j, out):
        out[...] = a_vm[pl.ds(pl.multiple_of(j * TN, TN), TN), :].T

    def transposed(aT):
        def body(idx, out):
            transpose_out(idx.index[0], out)
        pltpu.emit_pipeline(body, grid=(tokens // TN,), out_specs=[pl.BlockSpec((d, TN), lambda j: (0, j))], _explicit_indices=True)(aT)

    TM, TMD = 1024, 512

    def gate_up(at, width):
        def body(wg_t, wu_t, f_t, e_t, p_t):
            @pl.loop(0, tokens // TM)
            def _(i):
                rows = pl.ds(pl.multiple_of(i * TM, TM), TM)
                a = a_vm[rows, :]
                g = dot(a, wg_t[...])
                u = dot(a, wu_t[...])
                sig = jax.nn.sigmoid(g)
                s = g * sig
                f_t[rows, :] = s
                e_t[rows, :] = u * (sig + s * (1 - sig))
                p_t[rows, :] = (s * u).astype(BF16)
        j0 = at // TN
        w = pl.BlockSpec((d, TN), lambda j: (0, j + j0))
        o = pl.BlockSpec((tokens, TN), lambda j: (0, j + j0))
        pltpu.emit_pipeline(body, grid=(width // TN,), in_specs=[w, w], out_specs=[o, o, o])(WG.at[0], WU.at[0], f0, e0, p0)

    def down():
        c = pltpu.make_async_copy(WD.at[0], wd_vm, local.at[8])
        c.start()
        c.wait()

        def body(idx, p_t, x_t, h_t):
            y = dot(p_t[...], wd_vm[...]).astype(BF16)
            h = x_t[...] + y
            h_t[...] = h
            a_vm[pl.ds(pl.multiple_of(idx.index[0] * TMD, TMD), TMD), :] = rms(h)
        o = pl.BlockSpec((TMD, d), lambda i: (i, 0))
        pltpu.emit_pipeline(body, grid=(tokens // TMD,), in_specs=[pl.BlockSpec((TMD, ff), lambda i: (i, 0)), o], out_specs=[o], _explicit_indices=True)(p0, x, h1)

    def gate_up_back(events):
        def body(idx, wg_t, wu_t, wd_t, gd_t, dg_t, du_t):
            for at, what in events:
                pl.when(idx.index[0] == at)(what)

            @pl.loop(0, tokens // TM)
            def _(i):
                rows = pl.ds(pl.multiple_of(i * TM, TM), TM)
                a = a_vm[rows, :]
                g = dot(a, wg_t[...])
                u = dot(a, wu_t[...])
                dp = lax.dot_general(dy_vm[rows, :], wd_t[...], NT, preferred_element_type=F32).astype(BF16).astype(F32)
                sig = jax.nn.sigmoid(g)
                s = g * sig
                p_vm[rows, :] = (s * u).astype(BF16)
                du_t[rows, :] = (dp * s).astype(BF16)
                dg_t[rows, :] = (dp * u * (sig + s * (1 - sig))).astype(BF16)
            gd_t[...] = lax.dot_general(p_vm[...], dy_vm[...], TT, preferred_element_type=F32).astype(BF16)
        w = pl.BlockSpec((d, TN), lambda j: (0, j))
        o = pl.BlockSpec((tokens, TN), lambda j: (0, j))
        r = pl.BlockSpec((TN, d), lambda j: (j, 0))
        pltpu.emit_pipeline(body, grid=(ff // TN,), in_specs=[w, w, r], out_specs=[r, o, o], _explicit_indices=True)(
            WG.at[1], WU.at[1], WD.at[1], gd1, dg1, du1)

    transposed(a0T)
    for c in stores:
        c.wait()
    relay(0)
    n = len(units)

    def arrive(u):
        if u + 1 < n:
            relay(u + 1)
        last(u)
        complete(u)

    behind = [u for u, unit in enumerate(units) if unit[:2] == ("g", 1)]
    for u in range(behind[0] + 1):
        arrive(u)
        what, layer, at, width = units[u]
        if layer == 0 and what == "g":
            gate_up(at, width)
        elif layer == 0:
            down()
            transposed(a1T)
    gate_up_back([(units[u][2] // TN - 2, lambda u=u: arrive(u)) for u in behind[1:]])
    for i in range(len(pieces)):
        for kind in range(9):
            go(i, kind).wait_send()


def forward(x, dy, wg, wu, wd):
    tokens, d = x.shape
    ff = wg.shape[2]
    tiles = ff // TN
    a, b = (tiles + 1) // 2 * TN, tiles // 2 * TN
    units = [("g", 0, 0, a), ("g", 0, a, b), ("d", 0, 0, 0), ("d", 1, 0, 0)]
    at, sizes = 0, (3, 3, 4, 4)
    while at < ff:
        w = min((sizes[len(units) - 4] if len(units) < 8 else tiles) * TN, ff - at)
        units.append(("g", 1, at, w))
        at += w
    count = sum(2 if u[0] == "g" else 1 for u in units)
    big = jax.ShapeDtypeStruct((tokens, ff), BF16)
    wide = jax.ShapeDtypeStruct((tokens, ff), F32)
    h = jax.ShapeDtypeStruct((tokens, d), BF16)
    hT = jax.ShapeDtypeStruct((d, tokens), BF16)
    outs = [jax.ShapeDtypeStruct((2, d, ff), BF16)] * 2 + [jax.ShapeDtypeStruct((2, ff, d), BF16), wide, wide, big, h, hT, hT, jax.ShapeDtypeStruct((ff, d), BF16), big, big]

    def kernel(*refs):
        forward_kernel(units, tokens, d, ff, *refs)

    return pl.pallas_call(
        kernel,
        out_shape=outs,
        in_specs=[ANY] * 5,
        out_specs=[ANY] * len(outs),
        scratch_shapes=[
            pltpu.VMEM((tokens, d), BF16), pltpu.VMEM((tokens, d), BF16), pltpu.VMEM((ff, d), BF16), pltpu.VMEM((tokens, TN), BF16),
            pltpu.VMEM(wg.shape, BF16), pltpu.VMEM(wu.shape, BF16), pltpu.VMEM(wd.shape, BF16),
            pltpu.SemaphoreType.DMA((count, 9)), pltpu.SemaphoreType.DMA((count, 9)), pltpu.SemaphoreType.DMA((9,)),
        ],
        compiler_params=pltpu.CompilerParams(collective_id=0, has_side_effects=True, vmem_limit_bytes=60 * 2**20),
        name="forward",
    )(x, dy, wg, wu, wd)


class Unit:
    def __init__(self, n, slot, bufs, rows, width, by_rows, outs, older, newer, at=0):
        self.at = at
        self.n, self.slot, self.rows, self.width, self.by_rows, self.outs, self.older, self.newer = n, slot, rows, width, by_rows, outs, older, newer
        self.G, self.Rp, self.R1, self.R2 = bufs
        self.pieces = len(outs)
        self.h = (rows if by_rows else width) // 2

    def block(self, b):
        return self.G.at[:, pl.ds(pl.multiple_of(b * self.rows, 16), self.rows), pl.ds(self.at, self.width)]

    def half(self, b, part):
        if self.by_rows:
            return self.G.at[:, pl.ds(pl.multiple_of(b * self.rows + part * self.h, 16), self.h), pl.ds(self.at, self.width)]
        return self.G.at[:, pl.ds(pl.multiple_of(b * self.rows, 16), self.rows), pl.ds(part * self.h, self.h)]

    def narrow(self, ref):
        return ref.at[:, :, pl.ds(self.at, self.width) if self.by_rows else pl.ds(0, self.h)]

    def r1(self, part, which):
        return self.narrow(self.R1.at[part, which])

    def r2(self, part):
        return self.narrow(self.R2.at[part])

    def rp(self, q):
        return self.Rp.at[q, :, :, pl.ds(self.at, self.width)]


def backward_kernel(groups, tokens, d, ff, gd1, dg1, du1, a1T, dy, WG, WU, WD, h1, f0, e0, p0, a0T, gG, gU, gD,
                    aT_vm, dh_vm, Gg, Rpg, R1g, R2g, Gd, Rpd, R1d, R2d, send, recv, local, credit):
    me, flip = around()
    xn, yn, pn = flip(me, 4), flip(me, 2), flip(me, 1)
    core, q0 = me % 2, me // 2
    qx, qy = flip(q0, 2), flip(q0, 1)
    qd = flip(qx, 1)
    rg, rd = d // 8, ff // 8
    SLOTS = Gg.shape[0]

    barrier = pltpu.get_barrier_semaphore()
    for other in (xn, yn, pn):
        pl.semaphore_signal(barrier, inc=1, device_id={"dp": other}, device_id_type=pl.DeviceIdType.MESH)
    pl.semaphore_wait(barrier, 3)

    down_bufs = (Gd, Rpd, R1d, R2d)
    count = len(groups)
    D = {}
    for layer in (1, 0):
        for part, (at, width) in enumerate(((0, 512), (512, d - 512))):
            D[layer, part] = Unit(2 * count + 2 * layer + part, SLOTS + part, down_bufs, rd, width, True,
                                  [gD.at[layer, :, pl.ds(at, width)]], layer == 0, layer == 1, at)
    units = []
    for layer in (1, 0):
        for at, width in groups:
            n = len(units)
            s = n % SLOTS
            cols = pl.ds(at, width)
            units.append(Unit(n, s, (Gg.at[s], Rpg.at[s], R1g.at[s], R2g.at[s]), rg, width, False,
                              [gG.at[layer, :, cols], gU.at[layer, :, cols]], n >= SLOTS, n + SLOTS < 2 * count))

    def remote(u, k, src, dst, to):
        return pltpu.make_async_remote_copy(src_ref=src, dst_ref=dst, send_sem=send.at[u.n, k], recv_sem=recv.at[u.n, k],
                                            device_id={"dp": to}, device_id_type=pl.DeviceIdType.MESH)

    def to_partner(u, q):
        return remote(u, q, u.block(2 * q + 1 - core), u.rp(q), pn)

    def stage1(u, k):
        q, part, which, to = ((qd, 0, 1, xn), (qd, 1, 1, yn), (qx, 0, 0, xn), (qy, 1, 0, yn))[k]
        return remote(u, 4 + k, u.half(2 * q + core, part), u.r1(part, which), to)

    def stage2(u, k):
        q, to = ((qy, yn), (qx, xn))[k]
        return remote(u, 8 + k, u.half(2 * q + core, k), u.r2(k), to)

    def grant(u, k, to):
        pl.semaphore_signal(credit.at[u.slot, k], inc=1, device_id={"dp": to}, device_id_type=pl.DeviceIdType.MESH)

    def add(dst, *others):
        for i in range(dst.shape[0]):
            total = dst[i].astype(F32)
            for other in others:
                total = total + other[i].astype(F32)
            dst[i] = total.astype(BF16)

    def s0(u):
        if u.older:
            pl.semaphore_wait(credit.at[u.slot, 0], 1)
        for q in range(4):
            to_partner(u, q).start()

    def s1(u):
        for q in range(4):
            to_partner(u, q).wait_recv()

        @pl.loop(0, 4)
        def _(q):
            add(u.block(2 * q + core), u.rp(q))
        if u.newer:
            grant(u, 0, pn)
        if u.older:
            pl.semaphore_wait(credit.at[u.slot, 1], 1)
            pl.semaphore_wait(credit.at[u.slot, 2], 1)
        for k in range(4):
            stage1(u, k).start()

    def s2(u):
        stage1(u, 0).wait_recv()
        add(u.half(2 * qy + core, 0), u.r1(0, 1))
        stage2(u, 0).start()
        stage1(u, 1).wait_recv()
        add(u.half(2 * qx + core, 1), u.r1(1, 1))
        stage2(u, 1).start()

    def out(u, i):
        return pltpu.make_async_copy(u.block(me).at[i], u.outs[i], local.at[u.n, i])

    def s3(u):
        for k in (2, 3):
            stage1(u, k).wait_recv()
        for part in (0, 1):
            stage2(u, part).wait_recv()
            add(u.half(me, part), u.r1(part, 0), u.r2(part))
        for i in range(u.pieces):
            out(u, i).start()
        if u.newer:
            grant(u, 1, xn)
            grant(u, 2, yn)
        for q in range(4):
            to_partner(u, q).wait_send()
        for k in range(4):
            stage1(u, k).wait_send()
        for k in range(2):
            stage2(u, k).wait_send()

    def s4(u):
        for i in range(u.pieces):
            out(u, i).wait()

    def run(events, j):
        for at in sorted({e[0] for e in events}):
            @pl.when(j == at)
            def _(at=at):
                for when, what, u in events:
                    if when == at:
                        what(u)

    TM = 1024
    wide_tile = pl.BlockSpec((tokens, TN), lambda j: (0, j))
    w_tile = pl.BlockSpec((d, TN), lambda j: (0, j))

    def down_weight(p, cols, events):
        def body(idx, p_t):
            j = idx.index[0]
            run(events, j)
            g = lax.dot_general(p_t[...], dh_vm[:, cols], TT, preferred_element_type=F32)
            Gd[0, pl.ds(pl.multiple_of(j * TN, TN), TN), cols] = g.astype(BF16)
        pltpu.emit_pipeline(body, grid=(ff // TN,), in_specs=[wide_tile], _explicit_indices=True)(p)

    def store_weight(first, j, i, g_t):
        per = GROUP // TN
        slot = (j // per + first) % SLOTS
        off = pl.multiple_of((j % per) * TN, TN)
        Gg[slot, i, :, pl.ds(off, TN)] = dot(aT_vm[...], g_t[...]).astype(BF16)

    def layer1(acc, events):
        def body(idx, dg_t, du_t, wg_t, wu_t):
            j = idx.index[0]
            run(events, j)
            store_weight(0, j, 0, dg_t)
            store_weight(0, j, 1, du_t)
            value = lax.dot_general(dg_t[...], wg_t[...], NT, preferred_element_type=F32) + lax.dot_general(
                du_t[...], wu_t[...], NT, preferred_element_type=F32)
            acc[...] = jnp.where(j == 0, value, acc[...] + value)
        pltpu.emit_pipeline(body, grid=(ff // TN,), in_specs=[wide_tile, wide_tile, w_tile, w_tile], _explicit_indices=True)(dg1, du1, WG.at[1], WU.at[1])

        def norm(idx, h_t):
            rows = pl.ds(pl.multiple_of(idx.index[0] * TN, TN), TN)
            wide = h_t[...].astype(F32)
            da = acc[rows, :].astype(BF16).astype(F32)
            scale = lax.rsqrt(jnp.mean(wide * wide, -1, keepdims=True) + 1e-6)
            back = scale * (da - wide * (scale * scale * jnp.mean(da * wide, -1, keepdims=True)))
            dh_vm[rows, :] = dh_vm[rows, :] + back.astype(BF16)
        pltpu.emit_pipeline(norm, grid=(tokens // TN,), in_specs=[pl.BlockSpec((TN, d), lambda i: (i, 0))], _explicit_indices=True)(h1)

    def layer0(dg_vm, du_vm, events):
        def body(idx, wd_t, f_t, e_t):
            j = idx.index[0]
            run(events, j)

            @pl.loop(0, tokens // TM)
            def _(i):
                rows = pl.ds(pl.multiple_of(i * TM, TM), TM)
                dp = lax.dot_general(dh_vm[rows, :], wd_t[...], NT, preferred_element_type=F32).astype(BF16).astype(F32)
                du_vm[rows, :] = (dp * f_t[rows, :]).astype(BF16)
                dg_vm[rows, :] = (dp * e_t[rows, :]).astype(BF16)
            store_weight(count, j, 0, dg_vm)
            store_weight(count, j, 1, du_vm)
        pltpu.emit_pipeline(body, grid=(ff // TN,), in_specs=[pl.BlockSpec((TN, d), lambda j: (j, 0)), wide_tile, wide_tile], _explicit_indices=True)(
            WD.at[0], f0, e0)

    tiles = ff // TN
    order = {"L1": [], "Da": [], "Db": [], "L0": [], "end": []}
    LATER = 7

    def spot(tick):
        for name, ticks, step in (("L1", tiles, 1), ("Da", 4, 5), ("Db", 3, 6), ("L0", tiles, 1)):
            if tick < ticks:
                return name, tick * step
            tick -= ticks
        return "end", tick

    def plan(u, ticks):
        for tick, what in zip(ticks, (s0, s1, s2, s3, s4)):
            if tick is not None:
                where, at = spot(tick)
                order[where].append((at, what, u))

    plan(D[1, 0], (None, 1, 5, 8, 10))
    plan(D[1, 1], (2, 10, 14, 17, 19))
    for k, u in enumerate(units):
        at, width = groups[k % count]
        end = (at + width) // TN + (0 if k < count else tiles + LATER)
        plan(u, (end, end + 1, end + 5, end + 8, end + 9))
    start = tiles + 4
    plan(D[0, 0], (start, start + 1, start + 5, start + 8, start + 10))
    plan(D[0, 1], (start + 3, start + 4, start + 8, start + 11, start + 13))
    for events in order.values():
        events.sort(key=lambda e: (e[0], -(s0, s1, s2, s3, s4).index(e[1])))

    copies = [pltpu.make_async_copy(src, dst, local.at[0, k]) for k, (src, dst) in enumerate(((gd1, Gd.at[0]), (dy, dh_vm), (a1T, aT_vm)))]
    for c in copies:
        c.start()
    copies[0].wait()
    s0(D[1, 0])
    for c in copies[1:]:
        c.wait()
    pl.run_scoped(lambda acc: layer1(acc, order["L1"]), pltpu.VMEM((tokens, d), F32))
    c = pltpu.make_async_copy(a0T, aT_vm, local.at[0, 2])
    c.start()
    down_weight(p0, slice(0, 512), order["Da"])
    down_weight(p0, slice(512, d), order["Db"])
    c.wait()
    pl.run_scoped(lambda a, b: layer0(a, b, order["L0"]), pltpu.VMEM((tokens, TN), BF16), pltpu.VMEM((tokens, TN), BF16))
    for _, what, u in order["end"]:
        what(u)


def backward(gd1, dg1, du1, a1T, dy, WG, WU, WD, h1, f0, e0, p0, a0T):
    tokens, d = dy.shape
    ff = dg1.shape[1]
    tiles, groups, at = ff // TN, [], 0
    while at < ff:
        width = min(GROUP, ff - at)
        groups.append((at, width))
        at += width
    C, rg, rd, slots, n = GROUP, d // 8, ff // 8, 4, 2 * len(groups) + 4
    outs = [jax.ShapeDtypeStruct((2, rg, ff), BF16)] * 2 + [jax.ShapeDtypeStruct((2, rd, d), BF16)]

    def kernel(*refs):
        backward_kernel(groups, tokens, d, ff, *refs)

    return pl.pallas_call(
        kernel,
        out_shape=outs,
        in_specs=[ANY] * 13,
        out_specs=[ANY] * 3,
        scratch_shapes=[
            pltpu.VMEM((d, tokens), BF16), pltpu.VMEM((tokens, d), BF16),
            pltpu.VMEM((slots, 2, d, C), BF16), pltpu.VMEM((slots, 4, 2, rg, C), BF16),
            pltpu.VMEM((slots, 2, 2, 2, rg, C // 2), BF16), pltpu.VMEM((slots, 2, 2, rg, C // 2), BF16),
            pltpu.VMEM((1, ff, d), BF16), pltpu.VMEM((4, 1, rd, d), BF16),
            pltpu.VMEM((2, 2, 1, rd // 2, d), BF16), pltpu.VMEM((2, 1, rd // 2, d), BF16),
            pltpu.SemaphoreType.DMA((n, 10)), pltpu.SemaphoreType.DMA((n, 10)), pltpu.SemaphoreType.DMA((n, 3)),
            pltpu.SemaphoreType.REGULAR((slots + 2, 3)),
        ],
        compiler_params=pltpu.CompilerParams(collective_id=1, has_side_effects=True, vmem_limit_bytes=67000000),
        name="backward",
    )(gd1, dg1, du1, a1T, dy, WG, WU, WD, h1, f0, e0, p0, a0T)


def adamw(w, m, v, g):
    m = 0.9 * m + 0.1 * g
    v = 0.95 * v + 0.05 * g * g
    step = m * lax.rsqrt(v + 1e-8) + 0.1 * w
    return (w - 0.02 * step).astype(BF16), m, v


def solution(mesh):
    def step(x, dy, *arrays):
        weights, m, v = (arrays[i : i + 3] for i in (0, 3, 6))
        x, dy = x[0], dy[0]
        WG, WU, WD, f0, e0, p0, h1, a0T, a1T, gd1, dg1, du1 = forward(x, dy, *weights)
        gradients = [g.astype(F32) for g in backward(gd1, dg1, du1, a1T, dy, WG, WU, WD, h1, f0, e0, p0, a0T)]
        new = [adamw(w.astype(F32), m, v, g) for w, m, v, g in zip(weights, m, v, gradients, strict=True)]
        return tuple(one[which] for which in range(3) for one in new)

    states, cut = P(("rep", "dp"), None, None), P(None, "dp", None)
    return jax.shard_map(
        step,
        mesh=mesh,
        in_specs=(states, states) + (cut,) * 9,
        out_specs=(P("rep", "dp", None),) * 9,
        check_vma=False,
    )
```

```python
import jax
import jax.numpy as jnp
from jax import lax
from jax.experimental import pallas as pl
from jax.experimental.pallas import tpu as pltpu
from jax.sharding import PartitionSpec as P

NAMES = ("w_gate", "w_up", "w_down")
F32, BF16 = jnp.float32, jnp.bfloat16
TN = 256
GROUP = 3 * TN
ANY = pl.BlockSpec(memory_space=pl.ANY)
NT, TT = (((1,), (1,)), ((), ())), (((0,), (0,)), ((), ()))


def dot(a, b):
    return jnp.dot(a, b, preferred_element_type=F32)


def around():
    me = lax.axis_index("dp")

    def flip(i, bit):
        return i + bit - 2 * bit * ((i // bit) % 2)

    return me, flip


def rms(h):
    wide = h.astype(F32)
    return (wide * lax.rsqrt(jnp.mean(wide * wide, -1, keepdims=True) + 1e-6)).astype(BF16)


class Piece:
    def __init__(self, shard, full, layer, rows, columns=None):
        self.shard, self.full, self.layer, self.rows, self.columns = shard, full, layer, rows, columns

    def cut(self, part):
        if self.columns is None:
            n = self.rows if part is None else self.rows // 2
            return (n if part else 0), n, slice(None)
        at, width = self.columns
        n = width if part is None else width // 2
        return 0, self.rows, pl.ds(at + (n if part else 0), n)

    def own(self):
        off, n, cols = self.cut(None)
        return self.shard.at[self.layer, pl.ds(off, n), cols]

    def there(self, owner, part=None):
        off, n, cols = self.cut(part)
        return self.full.at[self.layer, pl.ds(pl.multiple_of(owner * self.rows + off, 16), n), cols]


def forward_kernel(units, tokens, d, ff, x, dy, wg, wu, wd, WG, WU, WD, f0, e0, p0, h1, a0, a1, gd1, dg1, du1,
                   a_vm, dy_vm, wd_vm, p_vm, own_g, own_u, own_d, send, recv, local):
    me, flip = around()
    xn, yn, pn = flip(me, 4), flip(me, 2), flip(me, 1)
    diag = flip(xn, 2)
    rg, rd = wg.shape[1], wd.shape[1]

    barrier = pltpu.get_barrier_semaphore()
    for other in (xn, yn, pn):
        pl.semaphore_signal(barrier, inc=1, device_id={"dp": other}, device_id_type=pl.DeviceIdType.MESH)
    pl.semaphore_wait(barrier, 3)

    pieces, of_unit = [], []
    for what, layer, at, width in units:
        mine = []
        if what == "g":
            mine = [Piece(wg, WG, layer, rg, (at, width)), Piece(wu, WU, layer, rg, (at, width))]
        else:
            mine = [Piece(wd, WD, layer, rd)]
        of_unit.append(range(len(pieces), len(pieces) + len(mine)))
        pieces += mine

    def go(i, kind):
        piece = pieces[i]
        src, dst, to = {
            0: (None, (me, None), xn),
            1: (None, (me, None), yn),
            2: (None, (me, None), pn),
            3: ((xn, 1), (xn, 1), yn),
            4: ((yn, 0), (yn, 0), xn),
            5: ((xn, None), (xn, None), pn),
            6: ((yn, None), (yn, None), pn),
            7: ((diag, 0), (diag, 0), pn),
            8: ((diag, 1), (diag, 1), pn),
        }[kind]
        return pltpu.make_async_remote_copy(
            src_ref=piece.own() if src is None else piece.there(*src), dst_ref=piece.there(*dst),
            send_sem=send.at[i, kind], recv_sem=recv.at[i, kind],
            device_id={"dp": to}, device_id_type=pl.DeviceIdType.MESH)

    def come(i, kind):
        owner, part, sender = {
            0: (xn, None, xn), 1: (yn, None, yn), 2: (pn, None, pn), 3: (diag, 1, yn), 4: (diag, 0, xn),
            5: (flip(pn, 4), None, pn), 6: (flip(pn, 2), None, pn), 7: (flip(diag, 1), 0, pn), 8: (flip(diag, 1), 1, pn),
        }[kind]
        ref = pieces[i].there(owner, part)
        pltpu.make_async_remote_copy(
            src_ref=ref, dst_ref=ref, send_sem=send.at[i, kind], recv_sem=recv.at[i, kind],
            device_id={"dp": sender}, device_id_type=pl.DeviceIdType.MESH).wait_recv()

    def first(u):
        for i in of_unit[u] if u < len(units) else ():
            for kind in (0, 1, 2):
                go(i, kind).start()

    def relay(u):
        for i in of_unit[u]:
            come(i, 0)
            go(i, 3).start()
            go(i, 5).start()
            come(i, 1)
            go(i, 4).start()
            go(i, 6).start()
        first(u + 2)

    def last(u):
        for i in of_unit[u]:
            come(i, 4)
            go(i, 7).start()
            come(i, 3)
            go(i, 8).start()

    def complete(u):
        for i in of_unit[u]:
            for kind in (2, 5, 6, 7, 8):
                come(i, kind)

    first(0)
    first(1)
    load = [pltpu.make_async_copy(s, t, local.at[k]) for k, (s, t) in enumerate(((x, a_vm), (dy, dy_vm), (wg, own_g), (wu, own_u), (wd, own_d)))]
    for c in load:
        c.start()
    load[0].wait()

    @pl.loop(0, tokens // TN)
    def _(i):
        rows = pl.ds(pl.multiple_of(i * TN, TN), TN)
        a_vm[rows, :] = rms(a_vm[rows, :])

    for c in load[1:]:
        c.wait()
    stores = []
    for k, (own, full, rows) in enumerate(((own_g, WG, rg), (own_u, WU, rg), (own_d, WD, rd))):
        c = pltpu.make_async_copy(own, full.at[:, pl.ds(pl.multiple_of(me * rows, 16), rows), :], local.at[5 + k])
        c.start()
        stores.append(c)

    TM, TMD = 1024, 512

    def gate_up(at, width):
        def body(wg_t, wu_t, f_t, e_t, p_t):
            @pl.loop(0, tokens // TM, unroll=True)
            def _(i):
                rows = pl.ds(pl.multiple_of(i * TM, TM), TM)
                a = a_vm[rows, :]
                g = dot(a, wg_t[...])
                u = dot(a, wu_t[...])
                sig = jax.nn.sigmoid(g)
                s = g * sig
                f_t[rows, :] = s
                e_t[rows, :] = u * (sig + s * (1 - sig))
                p_t[rows, :] = (s * u).astype(BF16)
        j0 = at // TN
        w = pl.BlockSpec((d, TN), lambda j: (0, j + j0))
        o = pl.BlockSpec((tokens, TN), lambda j: (0, j + j0))
        pltpu.emit_pipeline(body, grid=(width // TN,), in_specs=[w, w], out_specs=[o, o, o])(WG.at[0], WU.at[0], f0, e0, p0)

    def down():
        c = pltpu.make_async_copy(WD.at[0], wd_vm, local.at[10])
        c.start()
        c.wait()

        def body(idx, p_t, x_t, h_t):
            y = dot(p_t[...], wd_vm[...]).astype(BF16)
            h = x_t[...] + y
            h_t[...] = h
            a_vm[pl.ds(pl.multiple_of(idx.index[0] * TMD, TMD), TMD), :] = rms(h)
        o = pl.BlockSpec((TMD, d), lambda i: (i, 0))
        pltpu.emit_pipeline(body, grid=(tokens // TMD,), in_specs=[pl.BlockSpec((TMD, ff), lambda i: (i, 0)), o], out_specs=[o], _explicit_indices=True)(p0, x, h1)

    def gate_up_back(events):
        def body(idx, wg_t, wu_t, wd_t, gd_t, dg_t, du_t):
            for at, what in events:
                pl.when(idx.index[0] == at)(what)

            @pl.loop(0, tokens // TM, unroll=True)
            def _(i):
                rows = pl.ds(pl.multiple_of(i * TM, TM), TM)
                a = a_vm[rows, :]
                g = dot(a, wg_t[...])
                u = dot(a, wu_t[...])
                dp = lax.dot_general(dy_vm[rows, :], wd_t[...], NT, preferred_element_type=F32).astype(BF16).astype(F32)
                sig = jax.nn.sigmoid(g)
                s = g * sig
                p_vm[rows, :] = (s * u).astype(BF16)
                du_t[rows, :] = (dp * s).astype(BF16)
                dg_t[rows, :] = (dp * u * (sig + s * (1 - sig))).astype(BF16)
            gd_t[...] = lax.dot_general(p_vm[...], dy_vm[...], TT, preferred_element_type=F32).astype(BF16)
        w = pl.BlockSpec((d, TN), lambda j: (0, j))
        o = pl.BlockSpec((tokens, TN), lambda j: (0, j))
        r = pl.BlockSpec((TN, d), lambda j: (j, 0))
        pltpu.emit_pipeline(body, grid=(ff // TN,), in_specs=[w, w, r], out_specs=[r, o, o], _explicit_indices=True)(
            WG.at[1], WU.at[1], WD.at[1], gd1, dg1, du1)

    keep = [pltpu.make_async_copy(a_vm, a, local.at[8 + k]) for k, a in enumerate((a0, a1))]
    keep[0].start()
    for c in stores:
        c.wait()
    relay(0)
    n = len(units)

    def arrive(u):
        if u + 1 < n:
            relay(u + 1)
        last(u)
        complete(u)

    behind = [u for u, unit in enumerate(units) if unit[:2] == ("g", 1)]
    for u in range(behind[0] + 1):
        arrive(u)
        what, layer, at, width = units[u]
        if layer == 0 and what == "g":
            gate_up(at, width)
        elif layer == 0:
            keep[0].wait()
            down()
            keep[1].start()
    gate_up_back([(units[u][2] // TN - 2, lambda u=u: arrive(u)) for u in behind[1:]])
    keep[1].wait()
    for i in range(len(pieces)):
        for kind in range(9):
            go(i, kind).wait_send()


def forward(x, dy, wg, wu, wd):
    tokens, d = x.shape
    ff = wg.shape[2]
    tiles = ff // TN
    a, b = (tiles + 1) // 2 * TN, tiles // 2 * TN
    units = [("g", 0, 0, a), ("g", 0, a, b), ("d", 0, 0, 0), ("d", 1, 0, 0)]
    at, sizes = 0, (3, 3, 4, 4)
    while at < ff:
        w = min((sizes[len(units) - 4] if len(units) < 8 else tiles) * TN, ff - at)
        units.append(("g", 1, at, w))
        at += w
    count = sum(2 if u[0] == "g" else 1 for u in units)
    big = jax.ShapeDtypeStruct((tokens, ff), BF16)
    wide = jax.ShapeDtypeStruct((tokens, ff), F32)
    h = jax.ShapeDtypeStruct((tokens, d), BF16)
    outs = [jax.ShapeDtypeStruct((2, d, ff), BF16)] * 2 + [jax.ShapeDtypeStruct((2, ff, d), BF16), wide, wide, big, h, h, h, jax.ShapeDtypeStruct((ff, d), BF16), big, big]

    def kernel(*refs):
        forward_kernel(units, tokens, d, ff, *refs)

    return pl.pallas_call(
        kernel,
        out_shape=outs,
        in_specs=[ANY] * 5,
        out_specs=[ANY] * len(outs),
        scratch_shapes=[
            pltpu.VMEM((tokens, d), BF16), pltpu.VMEM((tokens, d), BF16), pltpu.VMEM((ff, d), BF16), pltpu.VMEM((tokens, TN), BF16),
            pltpu.VMEM(wg.shape, BF16), pltpu.VMEM(wu.shape, BF16), pltpu.VMEM(wd.shape, BF16),
            pltpu.SemaphoreType.DMA((count, 9)), pltpu.SemaphoreType.DMA((count, 9)), pltpu.SemaphoreType.DMA((11,)),
        ],
        compiler_params=pltpu.CompilerParams(collective_id=0, has_side_effects=True, vmem_limit_bytes=60 * 2**20),
        name="forward",
    )(x, dy, wg, wu, wd)


class Unit:
    def __init__(self, n, slot, bufs, rows, width, by_rows, outs, older, newer, at=0):
        self.at = at
        self.n, self.slot, self.rows, self.width, self.by_rows, self.outs, self.older, self.newer = n, slot, rows, width, by_rows, outs, older, newer
        self.G, self.Rp, self.R1, self.R2 = bufs
        self.pieces = len(outs)
        self.h = (rows if by_rows else width) // 2

    def block(self, b):
        return self.G.at[:, pl.ds(pl.multiple_of(b * self.rows, 16), self.rows), pl.ds(self.at, self.width)]

    def half(self, b, part):
        if self.by_rows:
            return self.G.at[:, pl.ds(pl.multiple_of(b * self.rows + part * self.h, 16), self.h), pl.ds(self.at, self.width)]
        return self.G.at[:, pl.ds(pl.multiple_of(b * self.rows, 16), self.rows), pl.ds(part * self.h, self.h)]

    def narrow(self, ref):
        return ref.at[:, :, pl.ds(self.at, self.width) if self.by_rows else pl.ds(0, self.h)]

    def r1(self, part, which):
        return self.narrow(self.R1.at[part, which])

    def r2(self, part):
        return self.narrow(self.R2.at[part])

    def rp(self, q):
        return self.Rp.at[q, :, :, pl.ds(self.at, self.width)]


def backward_kernel(groups, tokens, d, ff, gd1, dg1, du1, a1, dy, WG, WU, WD, h1, f0, e0, p0, a0, gG, gU, gD,
                    a_vm, dh_vm, Gg, Rpg, R1g, R2g, Gd, Rpd, R1d, R2d, send, recv, local, credit):
    me, flip = around()
    xn, yn, pn = flip(me, 4), flip(me, 2), flip(me, 1)
    core, q0 = me % 2, me // 2
    qx, qy = flip(q0, 2), flip(q0, 1)
    qd = flip(qx, 1)
    rg, rd = d // 8, ff // 8
    SLOTS = Gg.shape[0]

    barrier = pltpu.get_barrier_semaphore()
    for other in (xn, yn, pn):
        pl.semaphore_signal(barrier, inc=1, device_id={"dp": other}, device_id_type=pl.DeviceIdType.MESH)
    pl.semaphore_wait(barrier, 3)

    down_bufs = (Gd, Rpd, R1d, R2d)
    count = len(groups)
    D = {}
    for layer in (1, 0):
        for part, (at, width) in enumerate(((0, 512), (512, d - 512))):
            D[layer, part] = Unit(2 * count + 2 * layer + part, SLOTS + part, down_bufs, rd, width, True,
                                  [gD.at[layer, :, pl.ds(at, width)]], layer == 0, layer == 1, at)
    units = []
    for layer in (1, 0):
        for at, width in groups:
            n = len(units)
            s = n % SLOTS
            cols = pl.ds(at, width)
            units.append(Unit(n, s, (Gg.at[s], Rpg.at[s], R1g.at[s], R2g.at[s]), rg, width, False,
                              [gG.at[layer, :, cols], gU.at[layer, :, cols]], n >= SLOTS, n + SLOTS < 2 * count))

    def remote(u, k, src, dst, to):
        return pltpu.make_async_remote_copy(src_ref=src, dst_ref=dst, send_sem=send.at[u.n, k], recv_sem=recv.at[u.n, k],
                                            device_id={"dp": to}, device_id_type=pl.DeviceIdType.MESH)

    def to_partner(u, q):
        return remote(u, q, u.block(2 * q + 1 - core), u.rp(q), pn)

    def stage1(u, k):
        q, part, which, to = ((qd, 0, 1, xn), (qd, 1, 1, yn), (qx, 0, 0, xn), (qy, 1, 0, yn))[k]
        return remote(u, 4 + k, u.half(2 * q + core, part), u.r1(part, which), to)

    def stage2(u, k):
        q, to = ((qy, yn), (qx, xn))[k]
        return remote(u, 8 + k, u.half(2 * q + core, k), u.r2(k), to)

    def grant(u, k, to):
        pl.semaphore_signal(credit.at[u.slot, k], inc=1, device_id={"dp": to}, device_id_type=pl.DeviceIdType.MESH)

    def add(dst, *others):
        for i in range(dst.shape[0]):
            total = dst[i].astype(F32)
            for other in others:
                total = total + other[i].astype(F32)
            dst[i] = total.astype(BF16)

    def s0(u):
        if u.older:
            pl.semaphore_wait(credit.at[u.slot, 0], 1)
        for q in range(4):
            to_partner(u, q).start()

    def s1(u):
        for q in range(4):
            to_partner(u, q).wait_recv()

        @pl.loop(0, 4)
        def _(q):
            add(u.block(2 * q + core), u.rp(q))
        if u.newer:
            grant(u, 0, pn)
        if u.older:
            pl.semaphore_wait(credit.at[u.slot, 1], 1)
            pl.semaphore_wait(credit.at[u.slot, 2], 1)
        for k in range(4):
            stage1(u, k).start()

    def s2(u):
        stage1(u, 0).wait_recv()
        add(u.half(2 * qy + core, 0), u.r1(0, 1))
        stage2(u, 0).start()
        stage1(u, 1).wait_recv()
        add(u.half(2 * qx + core, 1), u.r1(1, 1))
        stage2(u, 1).start()

    def out(u, i):
        return pltpu.make_async_copy(u.block(me).at[i], u.outs[i], local.at[u.n, i])

    def s3(u):
        for k in (2, 3):
            stage1(u, k).wait_recv()
        for part in (0, 1):
            stage2(u, part).wait_recv()
            add(u.half(me, part), u.r1(part, 0), u.r2(part))
        for i in range(u.pieces):
            out(u, i).start()
        if u.newer:
            grant(u, 1, xn)
            grant(u, 2, yn)
        for q in range(4):
            to_partner(u, q).wait_send()
        for k in range(4):
            stage1(u, k).wait_send()
        for k in range(2):
            stage2(u, k).wait_send()

    def s4(u):
        for i in range(u.pieces):
            out(u, i).wait()

    def run(events, j):
        for at in sorted({e[0] for e in events}):
            @pl.when(j == at)
            def _(at=at):
                for when, what, u in events:
                    if when == at:
                        what(u)

    TM = 1024
    wide_tile = pl.BlockSpec((tokens, TN), lambda j: (0, j))
    w_tile = pl.BlockSpec((d, TN), lambda j: (0, j))

    def down_weight(p, cols, events):
        def body(idx, p_t):
            j = idx.index[0]
            run(events, j)
            g = lax.dot_general(p_t[...], dh_vm[:, cols], TT, preferred_element_type=F32)
            Gd[0, pl.ds(pl.multiple_of(j * TN, TN), TN), cols] = g.astype(BF16)
        pltpu.emit_pipeline(body, grid=(ff // TN,), in_specs=[wide_tile], _explicit_indices=True)(p)

    def store_weight(first, j, i, g_t):
        per = GROUP // TN
        slot = (j // per + first) % SLOTS
        off = pl.multiple_of((j % per) * TN, TN)
        Gg[slot, i, :, pl.ds(off, TN)] = lax.dot_general(a_vm[...], g_t[...], TT, preferred_element_type=F32).astype(BF16)

    def layer1(acc, events):
        def body(idx, dg_t, du_t, wg_t, wu_t):
            j = idx.index[0]
            run(events, j)
            store_weight(0, j, 0, dg_t)
            store_weight(0, j, 1, du_t)
            value = lax.dot_general(dg_t[...], wg_t[...], NT, preferred_element_type=F32) + lax.dot_general(
                du_t[...], wu_t[...], NT, preferred_element_type=F32)
            acc[...] = jnp.where(j == 0, value, acc[...] + value)
        pltpu.emit_pipeline(body, grid=(ff // TN,), in_specs=[wide_tile, wide_tile, w_tile, w_tile], _explicit_indices=True)(dg1, du1, WG.at[1], WU.at[1])

        def norm(idx, h_t):
            rows = pl.ds(pl.multiple_of(idx.index[0] * TN, TN), TN)
            wide = h_t[...].astype(F32)
            da = acc[rows, :].astype(BF16).astype(F32)
            scale = lax.rsqrt(jnp.mean(wide * wide, -1, keepdims=True) + 1e-6)
            back = scale * (da - wide * (scale * scale * jnp.mean(da * wide, -1, keepdims=True)))
            dh_vm[rows, :] = dh_vm[rows, :] + back.astype(BF16)
        pltpu.emit_pipeline(norm, grid=(tokens // TN,), in_specs=[pl.BlockSpec((TN, d), lambda i: (i, 0))], _explicit_indices=True)(h1)

    def layer0(dg_vm, du_vm, events):
        def body(idx, wd_t, f_t, e_t):
            j = idx.index[0]
            run(events, j)

            @pl.loop(0, tokens // TM, unroll=True)
            def _(i):
                rows = pl.ds(pl.multiple_of(i * TM, TM), TM)
                dp = lax.dot_general(dh_vm[rows, :], wd_t[...], NT, preferred_element_type=F32).astype(BF16).astype(F32)
                du_vm[rows, :] = (dp * f_t[rows, :]).astype(BF16)
                dg_vm[rows, :] = (dp * e_t[rows, :]).astype(BF16)
            store_weight(count, j, 0, dg_vm)
            store_weight(count, j, 1, du_vm)
        pltpu.emit_pipeline(body, grid=(ff // TN,), in_specs=[pl.BlockSpec((TN, d), lambda j: (j, 0)), wide_tile, wide_tile], _explicit_indices=True)(
            WD.at[0], f0, e0)

    tiles = ff // TN
    order = {"L1": [], "Da": [], "Db": [], "L0": [], "end": []}
    LATER = 7

    def spot(tick):
        for name, ticks, step in (("L1", tiles, 1), ("Da", 4, 5), ("Db", 3, 6), ("L0", tiles, 1)):
            if tick < ticks:
                return name, tick * step
            tick -= ticks
        return "end", tick

    def plan(u, ticks):
        for tick, what in zip(ticks, (s0, s1, s2, s3, s4)):
            if tick is not None:
                where, at = spot(tick)
                order[where].append((at, what, u))

    plan(D[1, 0], (None, 1, 5, 8, 10))
    plan(D[1, 1], (2, 10, 14, 17, 19))
    for k, u in enumerate(units):
        at, width = groups[k % count]
        end = (at + width) // TN + (0 if k < count else tiles + LATER)
        plan(u, (end, end + 1, end + 5, end + 8, end + 9))
    start = tiles + 4
    plan(D[0, 0], (start, start + 1, start + 5, start + 8, start + 10))
    plan(D[0, 1], (start + 3, start + 4, start + 8, start + 11, start + 13))
    for events in order.values():
        events.sort(key=lambda e: (e[0], -(s0, s1, s2, s3, s4).index(e[1])))

    copies = [pltpu.make_async_copy(src, dst, local.at[0, k]) for k, (src, dst) in enumerate(((gd1, Gd.at[0]), (dy, dh_vm), (a1, a_vm)))]
    for c in copies:
        c.start()
    copies[0].wait()
    s0(D[1, 0])
    for c in copies[1:]:
        c.wait()
    pl.run_scoped(lambda acc: layer1(acc, order["L1"]), pltpu.VMEM((tokens, d), F32))
    c = pltpu.make_async_copy(a0, a_vm, local.at[0, 2])
    c.start()
    down_weight(p0, slice(0, 512), order["Da"])
    down_weight(p0, slice(512, d), order["Db"])
    c.wait()
    pl.run_scoped(lambda a, b: layer0(a, b, order["L0"]), pltpu.VMEM((tokens, TN), BF16), pltpu.VMEM((tokens, TN), BF16))
    for _, what, u in order["end"]:
        what(u)


def backward(gd1, dg1, du1, a1, dy, WG, WU, WD, h1, f0, e0, p0, a0):
    tokens, d = dy.shape
    ff = dg1.shape[1]
    tiles, groups, at = ff // TN, [], 0
    while at < ff:
        width = min(GROUP, ff - at)
        groups.append((at, width))
        at += width
    C, rg, rd, slots, n = GROUP, d // 8, ff // 8, 4, 2 * len(groups) + 4
    outs = [jax.ShapeDtypeStruct((2, rg, ff), BF16)] * 2 + [jax.ShapeDtypeStruct((2, rd, d), BF16)]

    def kernel(*refs):
        backward_kernel(groups, tokens, d, ff, *refs)

    return pl.pallas_call(
        kernel,
        out_shape=outs,
        in_specs=[ANY] * 13,
        out_specs=[ANY] * 3,
        scratch_shapes=[
            pltpu.VMEM((tokens, d), BF16), pltpu.VMEM((tokens, d), BF16),
            pltpu.VMEM((slots, 2, d, C), BF16), pltpu.VMEM((slots, 4, 2, rg, C), BF16),
            pltpu.VMEM((slots, 2, 2, 2, rg, C // 2), BF16), pltpu.VMEM((slots, 2, 2, rg, C // 2), BF16),
            pltpu.VMEM((1, ff, d), BF16), pltpu.VMEM((4, 1, rd, d), BF16),
            pltpu.VMEM((2, 2, 1, rd // 2, d), BF16), pltpu.VMEM((2, 1, rd // 2, d), BF16),
            pltpu.SemaphoreType.DMA((n, 10)), pltpu.SemaphoreType.DMA((n, 10)), pltpu.SemaphoreType.DMA((n, 3)),
            pltpu.SemaphoreType.REGULAR((slots + 2, 3)),
        ],
        compiler_params=pltpu.CompilerParams(collective_id=1, has_side_effects=True, vmem_limit_bytes=67000000),
        name="backward",
    )(gd1, dg1, du1, a1, dy, WG, WU, WD, h1, f0, e0, p0, a0)


def adamw(w, m, v, g):
    m = 0.9 * m + 0.1 * g
    v = 0.95 * v + 0.05 * g * g
    step = m * lax.rsqrt(v + 1e-8) + 0.1 * w
    return (w - 0.02 * step).astype(BF16), m, v


def solution(mesh):
    def step(x, dy, *arrays):
        weights, m, v = (arrays[i : i + 3] for i in (0, 3, 6))
        x, dy = x[0], dy[0]
        WG, WU, WD, f0, e0, p0, h1, a0, a1, gd1, dg1, du1 = forward(x, dy, *weights)
        gradients = [g.astype(F32) for g in backward(gd1, dg1, du1, a1, dy, WG, WU, WD, h1, f0, e0, p0, a0)]
        new = [adamw(w.astype(F32), m, v, g) for w, m, v, g in zip(weights, m, v, gradients, strict=True)]
        return tuple(one[which] for which in range(3) for one in new)

    states, cut = P(("rep", "dp"), None, None), P(None, "dp", None)
    return jax.shard_map(
        step,
        mesh=mesh,
        in_specs=(states, states) + (cut,) * 9,
        out_specs=(P("rep", "dp", None),) * 9,
        check_vma=False,
    )
```
